16 devices in a mesh: dp: 2 (over y, z), ctx: 8 (over x, core).
Axes of the slice: x: 4, y: 2, z: 1, core: 2. Of those that a mesh axis runs over, the one named last changes fastest.
The devices are a block of a 4x4x8 slice.
Arguments:
- queries: bfloat16 [64, 1024, 8, 128], P('dp', 'ctx'), parts along dimension 0
- keys: bfloat16 [64, 1024, 1, 128], P('dp', 'ctx'), parts along dimension 0
- values: bfloat16 [64, 1024, 1, 128], P('dp', 'ctx'), parts along dimension 0
- grad_out: bfloat16 [64, 1024, 8, 128], P('dp', 'ctx'), parts along dimension 0
Outputs:
- output 1: bfloat16 [64, 1024, 8, 128], P('dp', 'ctx'), parts along dimension 0
- output 2: bfloat16 [64, 1024, 8, 128], P('dp', 'ctx'), parts along dimension 0
- output 3: bfloat16 [64, 1024, 1, 128], P('dp', 'ctx'), parts along dimension 0
- output 4: bfloat16 [64, 1024, 1, 128], P('dp', 'ctx'), parts along dimension 0
There are 2 independent parts. The reference program is written for one: setup_inputs(seed, part) draws one part's arguments, and reference() takes and returns one part's arrays. A program takes and returns all parts, laid end to end along the dimension named above; each array names one.
All inputs are finite; a program needn't handle non-finite values.
Results may differ from the reference program's by a relative error of at most 0.00671496.
Values are sent between devices in bfloat16 or wider.
A program may use at most 768 MiB of HBM per device.

```python
import jax
import jax.numpy as jnp
from jax import lax

BATCH = 32
SEQ = 1024
HQ = 8
HEAD_DIM = 128
BLOCK = 128
NEG_BIG = -1e30


def setup_inputs(seed: int = 0, part: int = 0) -> dict:
    part_key = jax.random.fold_in(jax.random.key(seed), part)
    key_q, key_k, key_v, key_do = jax.random.split(part_key, 4)
    q_shape = (BATCH, SEQ, HQ, HEAD_DIM)
    kv_shape = (BATCH, SEQ, 1, HEAD_DIM)
    queries = 1.5 * jax.random.normal(key_q, q_shape, jnp.float32)
    keys = jax.random.normal(key_k, kv_shape, jnp.float32)
    values = jax.random.normal(key_v, kv_shape, jnp.float32)
    grad_out = jax.random.normal(key_do, q_shape, jnp.float32)
    return {"queries": queries.astype(jnp.bfloat16), "keys": keys.astype(jnp.bfloat16), "values": values.astype(jnp.bfloat16), "grad_out": grad_out.astype(jnp.bfloat16)}


def reference(queries, keys, values, grad_out):
    n_kv = keys.shape[2]
    n_grp = HQ // n_kv
    n_blocks = SEQ // BLOCK
    scale = HEAD_DIM ** -0.5
    q_lead = jnp.moveaxis(queries.reshape(BATCH, n_blocks, BLOCK, n_kv, n_grp, HEAD_DIM), 1, 0)
    do_lead = jnp.moveaxis(grad_out.reshape(BATCH, n_blocks, BLOCK, n_kv, n_grp, HEAD_DIM), 1, 0)
    k_blocks = keys.reshape(BATCH, n_blocks, BLOCK, n_kv, HEAD_DIM)
    v_blocks = values.reshape(BATCH, n_blocks, BLOCK, n_kv, HEAD_DIM)
    blk_ids = jnp.arange(n_blocks)
    stat_shape = (BATCH, n_kv, n_grp, BLOCK)

    def block_scores(q_blk, k_blk, blk_idx, key_idx):
        scores = jnp.einsum("bihgd,bjhd->bhgij", q_blk.astype(jnp.float32), k_blk.astype(jnp.float32)) * scale
        q_pos = blk_idx * BLOCK + jnp.arange(BLOCK)
        k_pos = key_idx * BLOCK + jnp.arange(BLOCK)
        return jnp.where(q_pos[:, None] >= k_pos[None, :], scores, NEG_BIG)

    def forward_block(inputs):
        q_blk, blk_idx = inputs

        def loop_body(key_idx, carry):
            m_run, l_run, acc_run = carry
            k_blk = lax.dynamic_index_in_dim(k_blocks, key_idx, 1, keepdims=False)
            v_blk = lax.dynamic_index_in_dim(v_blocks, key_idx, 1, keepdims=False)
            scores = block_scores(q_blk, k_blk, blk_idx, key_idx)
            m_new = jnp.maximum(m_run, scores.max(axis=-1))
            rescale = jnp.exp(m_run - m_new)
            weights = jnp.exp(scores - m_new[..., None])
            l_new = l_run * rescale + weights.sum(axis=-1)
            w_half = weights.astype(jnp.bfloat16).astype(jnp.float32)
            acc_new = acc_run * rescale[..., None] + jnp.einsum("bhgij,bjhd->bhgid", w_half, v_blk.astype(jnp.float32))
            return m_new, l_new, acc_new

        init_carry = (jnp.full(stat_shape, NEG_BIG, jnp.float32), jnp.zeros(stat_shape, jnp.float32), jnp.zeros(stat_shape + (HEAD_DIM,), jnp.float32))
        m_fin, l_fin, acc_fin = lax.fori_loop(0, blk_idx + 1, loop_body, init_carry)
        out_blk = jnp.transpose((acc_fin / l_fin[..., None]).astype(jnp.bfloat16), (0, 3, 1, 2, 4))
        return out_blk, m_fin + jnp.log(l_fin)

    out_lead, lse_lead = lax.map(forward_block, (q_lead, blk_ids))

    def backward_block(carry, inputs):
        dk_acc, dv_acc = carry
        q_blk, do_blk, out_blk, lse_blk, blk_idx = inputs
        q_f = q_blk.astype(jnp.float32)
        do_f = do_blk.astype(jnp.float32)
        delta_row = jnp.einsum("bihgd,bihgd->bhgi", do_f, out_blk.astype(jnp.float32))

        def loop_body(key_idx, inner):
            dq_run, dk_run, dv_run = inner
            k_blk = lax.dynamic_index_in_dim(k_blocks, key_idx, 1, keepdims=False)
            v_blk = lax.dynamic_index_in_dim(v_blocks, key_idx, 1, keepdims=False)
            scores = block_scores(q_blk, k_blk, blk_idx, key_idx)
            weights = jnp.exp(scores - lse_blk[..., None])
            w_half = weights.astype(jnp.bfloat16).astype(jnp.float32)
            dp_blk = jnp.einsum("bihgd,bjhd->bhgij", do_f, v_blk.astype(jnp.float32))
            ds_half = (weights * (dp_blk - delta_row[..., None])).astype(jnp.bfloat16).astype(jnp.float32)
            dq_run = dq_run + jnp.einsum("bhgij,bjhd->bihgd", ds_half, k_blk.astype(jnp.float32))
            dk_old = lax.dynamic_index_in_dim(dk_run, key_idx, 1, keepdims=False)
            dv_old = lax.dynamic_index_in_dim(dv_run, key_idx, 1, keepdims=False)
            dk_new = dk_old + jnp.einsum("bhgij,bihgd->bjhd", ds_half, q_f)
            dv_new = dv_old + jnp.einsum("bhgij,bihgd->bjhd", w_half, do_f)
            dk_run = lax.dynamic_update_index_in_dim(dk_run, dk_new, key_idx, 1)
            dv_run = lax.dynamic_update_index_in_dim(dv_run, dv_new, key_idx, 1)
            return dq_run, dk_run, dv_run

        dq_blk, dk_acc, dv_acc = lax.fori_loop(0, blk_idx + 1, loop_body, (jnp.zeros(q_f.shape, jnp.float32), dk_acc, dv_acc))
        return (dk_acc, dv_acc), dq_blk

    acc_zero = jnp.zeros((BATCH, n_blocks, BLOCK, n_kv, HEAD_DIM), jnp.float32)
    grads, dq_lead = lax.scan(backward_block, (acc_zero, acc_zero), (q_lead, do_lead, out_lead, lse_lead, blk_ids))
    attn_out = jnp.moveaxis(out_lead, 0, 1).reshape(BATCH, SEQ, HQ, HEAD_DIM)
    grad_q = (jnp.moveaxis(dq_lead, 0, 1) * scale).astype(jnp.bfloat16).reshape(BATCH, SEQ, HQ, HEAD_DIM)
    grad_k = (grads[0] * scale).astype(jnp.bfloat16).reshape(BATCH, SEQ, n_kv, HEAD_DIM)
    grad_v = grads[1].astype(jnp.bfloat16).reshape(BATCH, SEQ, n_kv, HEAD_DIM)
    return attn_out, grad_q, grad_k, grad_v
```

```python
import functools
import math

import jax
import jax.numpy as jnp
from jax import lax
from jax.experimental import pallas as pl
from jax.experimental.pallas import tpu as pltpu
from jax.sharding import PartitionSpec as P

NEG_BIG = -1e30
CHUNK = 256
AHEAD = 4
FORWARD = 3
LAG = 2
NT = (((1,), (1,)), ((), ()))


def mm(a, b):
    return jnp.dot(a, b, preferred_element_type=jnp.float32)


def mm_nt(a, b):
    return lax.dot_general(a, b, NT, preferred_element_type=jnp.float32)


def attend(chip, t, grp, qd, kv, kvt, grads):
    c_len, d_head = kv.shape[-2:]
    pair = 2 * c_len
    rows = qd.shape[-2]
    scale = d_head ** -0.5
    k2 = scale * math.log2(math.e)
    n = chip + 1
    for j in range(n):
        kvt[j, 0] = kv[j, t, 0].reshape(pair, d_head).T
        kvt[j, 1] = kv[j, t, 1].reshape(pair, d_head).T
        grads[j, t] = jnp.zeros(grads.shape[2:], jnp.float32)
    toks = CHUNK // grp

    def chunk(r, _):
        rs = pl.ds(pl.multiple_of(r * CHUNK, CHUNK), CHUNK)
        qs = [qd[t, half, 0, rs] for half in range(2)]
        dos = [qd[t, half, 1, rs] for half in range(2)]
        pbs, dss = [], []
        for half in range(2):
            q, do = qs[half], dos[half]
            span = [pair] * chip + [c_len * (half + 1)]
            keys = [kv[j, t, 0].reshape(pair, d_head)[:span[j]] for j in range(n)]
            vals = [kv[j, t, 1].reshape(pair, d_head)[:span[j]] for j in range(n)]
            s = [mm_nt(k, q) for k in keys]
            dp = [mm_nt(v, do) for v in vals]
            tok = half * c_len + r * toks + lax.broadcasted_iota(jnp.int32, (1, CHUNK), 1) // grp
            key_pos = lax.broadcasted_iota(jnp.int32, (span[-1], CHUNK), 0)
            s[-1] = jnp.where(key_pos <= tok, s[-1], NEG_BIG)
            m = functools.reduce(jnp.maximum, [x.max(axis=0, keepdims=True) for x in s])
            mk = m * k2
            p = [jnp.exp2(x * k2 - mk) for x in s]
            rl = 1.0 / sum(x.sum(axis=0, keepdims=True) for x in p)
            p = [x * rl for x in p]
            pb = [x.astype(jnp.bfloat16) for x in p]
            o_t = sum(mm(kvt[j, 1, :, :span[j]], pb[j]) for j in range(n)).astype(jnp.bfloat16)
            delta = jnp.sum(do.T.astype(jnp.float32) * o_t.astype(jnp.float32), axis=0, keepdims=True)
            ds = [(x * (y - delta)).astype(jnp.bfloat16) for x, y in zip(p, dp)]
            dq_t = sum(mm(kvt[j, 0, :, :span[j]], ds[j]) for j in range(n)) * scale
            qd[t, half, 0, rs] = o_t.T
            qd[t, half, 1, rs] = dq_t.astype(jnp.bfloat16).T
            pbs.append(pb)
            dss.append(ds)
        for j in range(n):
            if j < chip:
                grads[j, t, 0] += mm(dss[0][j], qs[0]) + mm(dss[1][j], qs[1])
                grads[j, t, 1] += mm(pbs[0][j], dos[0]) + mm(pbs[1][j], dos[1])
            else:
                grads[j, t, 0] += mm(dss[1][j], qs[1])
                grads[j, t, 1] += mm(pbs[1][j], dos[1])
                grads[j, t, 0, :c_len] += mm(dss[0][j], qs[0])
                grads[j, t, 1, :c_len] += mm(pbs[0][j], dos[0])
        return 0

    lax.fori_loop(0, rows // CHUNK, chunk, 0)


def run_chip(chip, n_chip, grp, q_ref, do_ref, kv_ref, odq_ref, dkv_ref, qd, kv, kvt, grads, inbox,
             load_sem, pair_send, pair_recv, kv_send, kv_recv, fwd_send, sum_send, sum_recv,
             out_sem, out_send, out_recv, g_sem, g_send, g_recv):
    nb = qd.shape[0]
    c_len, d_head = kv.shape[-2:]
    scale = d_head ** -0.5
    core = lax.axis_index("ctx") % 2
    last = n_chip - 1
    targets = []
    if chip < last:
        targets.append(chip + 1)
    if chip == 0 and last > 1:
        targets.append(last)

    def dev(to_chip, to_core):
        return {"ctx": 2 * to_chip + to_core}

    def remote(src, dst, send, recv, to):
        return pltpu.make_async_remote_copy(src_ref=src, dst_ref=dst, send_sem=send, recv_sem=recv, device_id=to,
                                            device_id_type=pl.DeviceIdType.MESH)

    def loads(t):
        b = core * nb + t
        return [pltpu.make_async_copy(q_ref.at[b], qd.at[t, core, 0], load_sem.at[0, t]),
                pltpu.make_async_copy(do_ref.at[b], qd.at[t, core, 1], load_sem.at[1, t]),
                pltpu.make_async_copy(kv_ref.at[b], kv.at[chip, t, :, core], load_sem.at[2, t])]

    def pair_copies(t, half):
        b = (1 - core) * nb + t
        to = dev(chip, 1 - core)
        return [remote(q_ref.at[b], qd.at[t, half, 0], pair_send.at[0, t], pair_recv.at[0, t], to),
                remote(do_ref.at[b], qd.at[t, half, 1], pair_send.at[1, t], pair_recv.at[1, t], to),
                remote(kv_ref.at[b], kv.at[chip, t, :, half], pair_send.at[2, t], pair_recv.at[2, t], to)]

    def kv_pushes(t):
        out = []
        for i, to_chip in enumerate(targets):
            for other in range(2):
                plane = core if other == 0 else 1 - core
                out.append(remote(kv_ref.at[plane * nb + t], kv.at[chip, t, :, core], kv_send.at[i, other, t],
                                  kv_recv.at[chip, core, t], dev(to_chip, plane)))
        return out

    def direct(src):
        return src == chip - 1 or (src == 0 and chip == last)

    def kv_wait(src, t):
        if direct(src):
            for half in range(2):
                remote(kv_ref.at[0], kv.at[src, t, :, half], kv_send.at[0, 0, t], kv_recv.at[src, half, t],
                       dev(chip, 1 - core)).wait_recv()
        else:
            remote(kv.at[src, t], kv.at[src, t], fwd_send.at[0, t], kv_recv.at[src, 0, t], dev(chip, 1 - core)).wait_recv()

    fwd_srcs = [s for s in range(chip) if chip < last and not (s == 0 and chip + 1 == last)]

    def forward(i, t):
        src = fwd_srcs[i]
        return remote(kv.at[src, t], kv.at[src, t], fwd_send.at[i, t], kv_recv.at[src, 0, t], dev(chip + 1, core))

    def issue(t):
        for c in loads(t) + pair_copies(t, core) + kv_pushes(t):
            c.start()

    def issue_forward(t):
        for i, src in enumerate(fwd_srcs):
            kv_wait(src, t)
            forward(i, t).start()

    def send_sum(d, t):
        if chip == last and d == 0 and last > 1:
            to_chip, slot = 0, 0
        else:
            to_chip = chip - 1
            slot = 1 if d == to_chip else 0
        return remote(grads.at[d, t], inbox.at[slot, t], sum_send.at[d, t], sum_recv.at[slot, t], dev(to_chip, core))

    def inbox_wait(slot, t):
        remote(inbox.at[slot, t], inbox.at[slot, t], sum_send.at[0, t], sum_recv.at[slot, t],
               dev(chip, 1 - core)).wait_recv()

    merged = [d for d in range(chip) if chip < last and not (d == 0 and chip + 1 == last)]
    unmerged = [d for d in range(chip) if d not in merged]
    n_own = 0 if chip == last else (2 if (chip == 0 and last > 1) else 1)

    def outs(t):
        b = core * nb + t
        return [pltpu.make_async_copy(qd.at[t, core], odq_ref.at[b], out_sem.at[t]),
                remote(qd.at[t, 1 - core], odq_ref.at[b], out_send.at[t], out_recv.at[t], dev(chip, 1 - core))]

    def grad_outs(t):
        b = core * nb + t
        return [pltpu.make_async_copy(kv.at[chip, t, :, core], dkv_ref.at[b], g_sem.at[t]),
                remote(kv.at[chip, t, :, 1 - core], dkv_ref.at[b], g_send.at[t], g_recv.at[t], dev(chip, 1 - core))]

    def reduce_step(t):
        for d in merged:
            inbox_wait(0, t)
            grads[d, t] += inbox[0, t]
            send_sum(d, t).start()
        total = grads[chip, t]
        if n_own >= 1:
            inbox_wait(1, t)
            total = total + inbox[1, t]
        if n_own == 2:
            inbox_wait(0, t)
            total = total + inbox[0, t]
        block = (2, c_len, d_head)
        kv[chip, t, 0] = (total[0] * scale).astype(jnp.bfloat16).reshape(block)
        kv[chip, t, 1] = total[1].astype(jnp.bfloat16).reshape(block)
        for c in grad_outs(t):
            c.start()

    lag = LAG * (last - chip)

    def prologue(t, _):
        issue(t)
        return 0

    lax.fori_loop(0, AHEAD, prologue, 0)
    if fwd_srcs:
        def fwd_prologue(t, _):
            issue_forward(t)
            return 0
        lax.fori_loop(0, FORWARD, fwd_prologue, 0)

    def step(t, _):
        @pl.when(t + AHEAD < nb)
        def _():
            issue(t + AHEAD)
        if fwd_srcs:
            @pl.when(t + FORWARD < nb)
            def _():
                issue_forward(t + FORWARD)
        for c in loads(t):
            c.wait()
        for c in pair_copies(t, 1 - core):
            c.wait_recv()
        for src in range(chip):
            if src not in fwd_srcs:
                kv_wait(src, t)
        attend(chip, t, grp, qd, kv, kvt, grads)
        for c in outs(t):
            c.start()
        for d in unmerged[::-1]:
            send_sum(d, t).start()
        @pl.when(t >= lag)
        def _():
            reduce_step(t - lag)
        return 0

    lax.fori_loop(0, nb, step, 0)

    def tail(t, _):
        reduce_step(t)
        return 0

    if lag:
        lax.fori_loop(nb - lag, nb, tail, 0)

    def drain(t, _):
        for c in pair_copies(t, core) + kv_pushes(t):
            c.wait_send()
        for i in range(len(fwd_srcs)):
            forward(i, t).wait_send()
        for d in range(chip):
            send_sum(d, t).wait_send()
        b = (1 - core) * nb + t
        for local, away in (outs(t), grad_outs(t)):
            local.wait()
            away.wait_send()
        remote(qd.at[t, core], odq_ref.at[b], out_send.at[t], out_recv.at[t], dev(chip, 1 - core)).wait_recv()
        remote(kv.at[chip, t, :, core], dkv_ref.at[b], g_send.at[t], g_recv.at[t], dev(chip, 1 - core)).wait_recv()
        return 0

    lax.fori_loop(0, nb, drain, 0)


def kernel(n_chip, grp, *refs):
    me = lax.axis_index("ctx")
    barrier = pltpu.get_barrier_semaphore()
    for i in range(1, 2 * n_chip):
        pl.semaphore_signal(barrier, inc=1, device_id={"ctx": lax.rem(me + i, 2 * n_chip)},
                            device_id_type=pl.DeviceIdType.MESH)
    pl.semaphore_wait(barrier, 2 * n_chip - 1)
    for chip in range(n_chip):
        @pl.when(me // 2 == chip)
        def _():
            run_chip(chip, n_chip, grp, *refs)


def solution(mesh):
    part_spec = P("dp", "ctx")
    n_chip = mesh.shape["ctx"] // 2

    def local_step(queries, keys, values, grad_out):
        n_batch, c_len, n_q, d_head = queries.shape
        rows = c_len * n_q
        nb = n_batch // 2
        q = queries.reshape(n_batch, rows, d_head)
        do = grad_out.reshape(n_batch, rows, d_head)
        kv = jnp.stack([keys.reshape(n_batch, c_len, d_head), values.reshape(n_batch, c_len, d_head)], axis=1)
        dma = pltpu.SemaphoreType.DMA
        any_spec = pl.BlockSpec(memory_space=pl.ANY)
        pairs = n_chip
        flops = 2 * nb * 2 * rows * n_chip * 2 * c_len * d_head * 6
        odq, dkv = pl.pallas_call(
            functools.partial(kernel, n_chip, n_q),
            in_specs=[any_spec] * 3,
            out_specs=[any_spec] * 2,
            out_shape=[jax.ShapeDtypeStruct((n_batch, 2, rows, d_head), jnp.bfloat16),
                       jax.ShapeDtypeStruct((n_batch, 2, c_len, d_head), jnp.bfloat16)],
            scratch_shapes=[
                pltpu.VMEM((nb, 2, 2, rows, d_head), jnp.bfloat16),
                pltpu.VMEM((pairs, nb, 2, 2, c_len, d_head), jnp.bfloat16),
                pltpu.VMEM((pairs, 2, d_head, 2 * c_len), jnp.bfloat16),
                pltpu.VMEM((pairs, nb, 2, 2 * c_len, d_head), jnp.float32),
                pltpu.VMEM((2, nb, 2, 2 * c_len, d_head), jnp.float32),
                dma((3, nb)), dma((3, nb)), dma((3, nb)),
                dma((2, 2, nb)), dma((pairs, 2, nb)), dma((max(pairs - 2, 1), nb)),
                dma((pairs, nb)), dma((2, nb)),
                dma((nb,)), dma((nb,)), dma((nb,)),
                dma((nb,)), dma((nb,)), dma((nb,)),
            ],
            compiler_params=pltpu.CompilerParams(vmem_limit_bytes=67043328, collective_id=0, has_side_effects=True),
            cost_estimate=pl.CostEstimate(flops=flops, bytes_accessed=4 * q.size * 2, transcendentals=0),
        )(q, do, kv)
        shape, kv_shape = queries.shape, keys.shape
        return (odq[:, 0].reshape(shape), odq[:, 1].reshape(shape),
                dkv[:, 0].reshape(kv_shape), dkv[:, 1].reshape(kv_shape))

    return jax.shard_map(local_step, mesh=mesh, in_specs=(part_spec,) * 4, out_specs=(part_spec,) * 4, check_vma=False)
```

```python
import functools
import math

import jax
import jax.numpy as jnp
from jax import lax
from jax.experimental import pallas as pl
from jax.experimental.pallas import tpu as pltpu
from jax.sharding import PartitionSpec as P

NEG_BIG = -1e30
CHUNK = 512
EARLY = 2
AHEAD = 3
FORWARD = 2
NT = (((1,), (1,)), ((), ()))


def mm(a, b):
    return jnp.dot(a, b, preferred_element_type=jnp.float32)


def mm_nt(a, b):
    return lax.dot_general(a, b, NT, preferred_element_type=jnp.float32)


def grad_parts(chip, half, t, bufs, grads):
    pbs, dss, rows_buf = bufs
    c_len = grads.shape[3] // 2

    def part(j, which, buf):
        span = slice(None) if half or j < chip else slice(0, c_len)

        def run():
            grads[j, t, which, span] += mm(buf[half, j, span], rows_buf[half, which])
        return run

    return [part(j, which, buf) for j in range(chip + 1) for which, buf in ((1, pbs), (0, dss))]


def softmax_part(chip, half, r, t, grp, qd, kv, kvt, bufs, fill):
    pbs, dss, rows_buf = bufs
    c_len, d_head = kv.shape[-2:]
    pair = 2 * c_len
    scale = d_head ** -0.5
    k2 = scale * math.log2(math.e)
    n = chip + 1
    fill = list(fill)
    rs = pl.ds(pl.multiple_of(r * CHUNK, CHUNK), CHUNK)
    q = qd[t, half, 0, rs]
    do = qd[t, half, 1, rs]
    rows_buf[half, 0] = q
    rows_buf[half, 1] = do
    span = [pair] * chip + [c_len * (half + 1)]
    tops = [pair * j for j in range(n)]
    n_key = sum(span)
    keys = kv[:n, t, 0].reshape(n * pair, d_head)[:n_key]
    vals = kv[:n, t, 1].reshape(n * pair, d_head)[:n_key]
    s_all = mm_nt(keys, q)
    s = [s_all[a:a + w] for a, w in zip(tops, span)]
    tok = half * c_len + r * (CHUNK // grp) + lax.broadcasted_iota(jnp.int32, (1, CHUNK), 1) // grp
    key_pos = lax.broadcasted_iota(jnp.int32, (span[-1], CHUNK), 0)
    s[-1] = jnp.where(key_pos <= tok, s[-1], NEG_BIG)
    m = functools.reduce(jnp.maximum, [x.max(axis=0, keepdims=True) for x in s])
    mk = m * k2
    p = []
    l = 0.0
    for j in range(n):
        parts = []
        for a in range(0, span[j], c_len):
            x = jnp.exp2(s[j][a:a + c_len] * k2 - mk)
            l = l + x.sum(axis=0, keepdims=True)
            parts.append(x)
            if fill:
                fill.pop(0)()
        p.append(parts)
    for step in fill:
        step()
    rl = 1.0 / l
    o_t = None
    for j in range(n):
        for i, x in enumerate(p[j]):
            pbs[half, j, i * c_len:(i + 1) * c_len] = (x * rl).astype(jnp.bfloat16)
        part = mm(kvt[j, 1, :, :span[j]], pbs[half, j, :span[j]])
        o_t = part if o_t is None else o_t + part
    dps = [mm_nt(vals[a:a + w], do) for a, w in list(zip(tops, span))[:EARLY]]
    o_t = o_t.astype(jnp.bfloat16)
    delta = jnp.sum(do.T.astype(jnp.float32) * o_t.astype(jnp.float32), axis=0, keepdims=True)
    dq_t = None
    for j in range(n):
        if j + EARLY < n:
            a = tops[j + EARLY]
            dps.append(mm_nt(vals[a:a + span[j + EARLY]], do))
        for i, x in enumerate(p[j]):
            at = slice(i * c_len, (i + 1) * c_len)
            dss[half, j, at] = (x * rl * (dps[j][at] - delta)).astype(jnp.bfloat16)
        part = mm(kvt[j, 0, :, :span[j]], dss[half, j, :span[j]])
        dq_t = part if dq_t is None else dq_t + part
    qd[t, half, 0, rs] = o_t.T
    qd[t, half, 1, rs] = (dq_t * scale).astype(jnp.bfloat16).T


def attend(chip, t, grp, qd, kv, kvt, grads, bufs, send_now):
    c_len, d_head = kv.shape[-2:]
    pair = 2 * c_len
    nb = qd.shape[0]
    for j in range(chip + 1):
        kvt[j, 0] = kv[j, t, 0].reshape(pair, d_head).T
        kvt[j, 1] = kv[j, t, 1].reshape(pair, d_head).T
        grads[j, t] = jnp.zeros(grads.shape[2:], jnp.float32)

    def chunk(r, _):
        before = jnp.where(r == 0, jnp.maximum(t - 1, 0), t)
        softmax_part(chip, 0, r, t, grp, qd, kv, kvt, bufs, grad_parts(chip, 1, before, bufs, grads))

        @pl.when((r == 0) & (t >= 1))
        def _():
            send_now(t - 1)

        @pl.when(t < nb)
        def _():
            softmax_part(chip, 1, r, t, grp, qd, kv, kvt, bufs, grad_parts(chip, 0, t, bufs, grads))
        return 0

    lax.fori_loop(0, qd.shape[-2] // CHUNK, chunk, 0)


NOW = {0: ((), ()), 1: (((0, 0, 1),), ()), 2: (((0, 3, 0),), ((1, 1, 1), (0, 1, 0))),
       3: (((1, 2, 0), (2, 2, 1)), ((1, 0, 2), (0, 0, 0), (2, 2, 1)))}
MERGED = {0: (None, None), 1: (None, (0, 0, 1)), 2: ((1, 1, 1), None), 3: ((0, 0, 0), None)}
OWN_SLOTS = {0: (1, 0), 1: (1,), 2: (1,), 3: ()}
LAGS = {0: 7, 1: 5, 2: 3, 3: 3}


def run_chip(chip, n_chip, grp, q_ref, do_ref, kv_ref, odq_ref, dkv_ref, qd, kv, kvt, grads, inbox, relay,
             pbs, dss, rows_buf, load_sem, pair_send, pair_recv, kv_send, kv_recv, fwd_send, sum_send, sum_recv,
             relay_send, relay_recv,
             out_sem, out_send, out_recv, g_sem, g_send, g_recv):
    nb = qd.shape[0]
    c_len, d_head = kv.shape[-2:]
    scale = d_head ** -0.5
    core = lax.axis_index("ctx") % 2
    last = n_chip - 1
    targets = []
    if chip < last:
        targets.append(chip + 1)
    if chip == 0 and last > 1:
        targets.append(last)

    def dev(to_chip, to_core):
        return {"ctx": 2 * to_chip + to_core}

    def remote(src, dst, send, recv, to):
        return pltpu.make_async_remote_copy(src_ref=src, dst_ref=dst, send_sem=send, recv_sem=recv, device_id=to,
                                            device_id_type=pl.DeviceIdType.MESH)

    def loads(t):
        b = core * nb + t
        return [pltpu.make_async_copy(q_ref.at[b], qd.at[t, core, 0], load_sem.at[0, t]),
                pltpu.make_async_copy(do_ref.at[b], qd.at[t, core, 1], load_sem.at[1, t]),
                pltpu.make_async_copy(kv_ref.at[b], kv.at[chip, t, :, core], load_sem.at[2, t])]

    def pair_copies(t, half):
        b = (1 - core) * nb + t
        to = dev(chip, 1 - core)
        return [remote(q_ref.at[b], qd.at[t, half, 0], pair_send.at[0, t], pair_recv.at[0, t], to),
                remote(do_ref.at[b], qd.at[t, half, 1], pair_send.at[1, t], pair_recv.at[1, t], to),
                remote(kv_ref.at[b], kv.at[chip, t, :, half], pair_send.at[2, t], pair_recv.at[2, t], to)]

    def kv_pushes(t):
        out = []
        for i, to_chip in enumerate(targets):
            for other in range(2):
                plane = core if other == 0 else 1 - core
                out.append(remote(kv_ref.at[plane * nb + t], kv.at[chip, t, :, core], kv_send.at[i, other, t],
                                  kv_recv.at[chip, core, t], dev(to_chip, plane)))
        return out

    def direct(src):
        return src == chip - 1 or (src == 0 and chip == last)

    def kv_wait(src, t):
        if direct(src):
            for half in range(2):
                remote(kv_ref.at[0], kv.at[src, t, :, half], kv_send.at[0, 0, t], kv_recv.at[src, half, t],
                       dev(chip, 1 - core)).wait_recv()
        else:
            remote(kv.at[src, t], kv.at[src, t], fwd_send.at[0, t], kv_recv.at[src, 0, t], dev(chip, 1 - core)).wait_recv()

    fwd_srcs = [s for s in range(chip) if chip < last and not (s == 0 and chip + 1 == last)]

    def forward(i, t):
        src = fwd_srcs[i]
        return remote(kv.at[src, t], kv.at[src, t], fwd_send.at[i, t], kv_recv.at[src, 0, t], dev(chip + 1, core))

    def issue(t):
        for c in loads(t) + pair_copies(t, core) + kv_pushes(t):
            c.start()

    def issue_forward(t):
        for i, src in enumerate(fwd_srcs):
            kv_wait(src, t)
            forward(i, t).start()

    def send_sum(route, t):
        d, to_chip, slot = route
        if slot == 2:
            dst, recv = relay.at[t // 2], relay_recv.at[t // 2]
        else:
            dst, recv = inbox.at[slot, t], sum_recv.at[slot, t]
        return remote(grads.at[d, t], dst, sum_send.at[d, t], recv, dev(to_chip, core))

    def relay_on(t):
        u = t // 2
        return remote(relay.at[u], relay.at[u], relay_send.at[u], relay_recv.at[u], dev(1, core))

    def inbox_wait(slot, t):
        remote(inbox.at[slot, t], inbox.at[slot, t], sum_send.at[0, t], sum_recv.at[slot, t],
               dev(chip, 1 - core)).wait_recv()

    def by_parity(t, even, odd):
        for parity, body in enumerate((even, odd)):
            if body is not None:
                pl.when(t % 2 == parity)(body)

    def outs(t):
        b = core * nb + t
        return [pltpu.make_async_copy(qd.at[t, core], odq_ref.at[b], out_sem.at[t]),
                remote(qd.at[t, 1 - core], odq_ref.at[b], out_send.at[t], out_recv.at[t], dev(chip, 1 - core))]

    def grad_outs(t):
        b = core * nb + t
        return [pltpu.make_async_copy(kv.at[chip, t, :, core], dkv_ref.at[b], g_sem.at[t]),
                remote(kv.at[chip, t, :, 1 - core], dkv_ref.at[b], g_send.at[t], g_recv.at[t], dev(chip, 1 - core))]

    def send_now(t):
        def body(routes):
            def start():
                for route in routes:
                    send_sum(route, t).start()
            return start if routes else None
        by_parity(t, *map(body, NOW[chip]))

    def merge(t):
        def body(route):
            def pass_on():
                inbox_wait(0, t)
                grads[route[0], t] += inbox[0, t]
                send_sum(route, t).start()
            return pass_on if route else None
        by_parity(t, *map(body, MERGED[chip]))
        if chip < 2:
            def relayed():
                relay_on(t).wait_recv()
                if chip == 0:
                    relay_on(t).start()
                else:
                    grads[chip, t] += relay[t // 2]
            by_parity(t, None, relayed)

    def reduce_step(t):
        merge(t)
        total = grads[chip, t]
        for slot in OWN_SLOTS[chip]:
            inbox_wait(slot, t)
            total = total + inbox[slot, t]
        block = (2, c_len, d_head)
        kv[chip, t, 0] = (total[0] * scale).astype(jnp.bfloat16).reshape(block)
        kv[chip, t, 1] = total[1].astype(jnp.bfloat16).reshape(block)
        for c in grad_outs(t):
            c.start()

    lag = LAGS[chip]
    bufs = (pbs, dss, rows_buf)
    for ref in bufs:
        ref[...] = jnp.zeros(ref.shape, ref.dtype)

    def prologue(t, _):
        issue(t)
        return 0

    lax.fori_loop(0, AHEAD, prologue, 0)
    if fwd_srcs:
        def fwd_prologue(t, _):
            issue_forward(t)
            return 0
        lax.fori_loop(0, FORWARD, fwd_prologue, 0)

    def step(t, _):
        @pl.when(t + AHEAD < nb)
        def _():
            issue(t + AHEAD)
        if fwd_srcs:
            @pl.when(t + FORWARD < nb)
            def _():
                issue_forward(t + FORWARD)
        for c in loads(t):
            c.wait()
        for c in pair_copies(t, 1 - core):
            c.wait_recv()
        for src in range(chip):
            if src not in fwd_srcs:
                kv_wait(src, t)
        attend(chip, t, grp, qd, kv, kvt, grads, bufs, send_now)
        for c in outs(t):
            c.start()

        @pl.when(t >= lag)
        def _():
            reduce_step(t - lag)
        return 0

    lax.fori_loop(0, nb, step, 0)
    for part in grad_parts(chip, 1, nb - 1, bufs, grads):
        part()
    send_now(nb - 1)

    def tail(t, _):
        reduce_step(t)
        return 0

    lax.fori_loop(nb - lag, nb, tail, 0)

    def drain(t, _):
        for c in pair_copies(t, core) + kv_pushes(t):
            c.wait_send()
        for i in range(len(fwd_srcs)):
            forward(i, t).wait_send()
        def sent(now, merged, parity):
            routes = now + ((merged,) if merged else ())
            relays = chip == 0 and parity == 1

            def wait():
                for route in routes:
                    send_sum(route, t).wait_send()
                if relays:
                    relay_on(t).wait_send()
            return wait if routes or relays else None
        by_parity(t, *(sent(NOW[chip][i], MERGED[chip][i], i) for i in range(2)))
        b = (1 - core) * nb + t
        for local, away in (outs(t), grad_outs(t)):
            local.wait()
            away.wait_send()
        remote(qd.at[t, core], odq_ref.at[b], out_send.at[t], out_recv.at[t], dev(chip, 1 - core)).wait_recv()
        remote(kv.at[chip, t, :, core], dkv_ref.at[b], g_send.at[t], g_recv.at[t], dev(chip, 1 - core)).wait_recv()
        return 0

    lax.fori_loop(0, nb, drain, 0)


def kernel(n_chip, grp, *refs):
    me = lax.axis_index("ctx")
    barrier = pltpu.get_barrier_semaphore()
    for i in range(1, 2 * n_chip):
        pl.semaphore_signal(barrier, inc=1, device_id={"ctx": lax.rem(me + i, 2 * n_chip)},
                            device_id_type=pl.DeviceIdType.MESH)
    pl.semaphore_wait(barrier, 2 * n_chip - 1)
    for chip in range(n_chip):
        @pl.when(me // 2 == chip)
        def _():
            run_chip(chip, n_chip, grp, *refs)


def solution(mesh):
    part_spec = P("dp", "ctx")
    n_chip = mesh.shape["ctx"] // 2

    def local_step(queries, keys, values, grad_out):
        n_batch, c_len, n_q, d_head = queries.shape
        rows = c_len * n_q
        nb = n_batch // 2
        q = queries.reshape(n_batch, rows, d_head)
        do = grad_out.reshape(n_batch, rows, d_head)
        kv = jnp.stack([keys.reshape(n_batch, c_len, d_head), values.reshape(n_batch, c_len, d_head)], axis=1)
        dma = pltpu.SemaphoreType.DMA
        any_spec = pl.BlockSpec(memory_space=pl.ANY)
        pairs = n_chip
        flops = 2 * nb * 2 * rows * n_chip * 2 * c_len * d_head * 6
        odq, dkv = pl.pallas_call(
            functools.partial(kernel, n_chip, n_q),
            in_specs=[any_spec] * 3,
            out_specs=[any_spec] * 2,
            out_shape=[jax.ShapeDtypeStruct((n_batch, 2, rows, d_head), jnp.bfloat16),
                       jax.ShapeDtypeStruct((n_batch, 2, c_len, d_head), jnp.bfloat16)],
            scratch_shapes=[
                pltpu.VMEM((nb, 2, 2, rows, d_head), jnp.bfloat16),
                pltpu.VMEM((pairs, nb, 2, 2, c_len, d_head), jnp.bfloat16),
                pltpu.VMEM((pairs, 2, d_head, 2 * c_len), jnp.bfloat16),
                pltpu.VMEM((pairs, nb, 2, 2 * c_len, d_head), jnp.float32),
                pltpu.VMEM((2, nb, 2, 2 * c_len, d_head), jnp.float32),
                pltpu.VMEM((nb // 2, 2, 2 * c_len, d_head), jnp.float32),
                pltpu.VMEM((2, pairs, 2 * c_len, CHUNK), jnp.bfloat16),
                pltpu.VMEM((2, pairs, 2 * c_len, CHUNK), jnp.bfloat16),
                pltpu.VMEM((2, 2, CHUNK, d_head), jnp.bfloat16),
                dma((3, nb)), dma((3, nb)), dma((3, nb)),
                dma((2, 2, nb)), dma((pairs, 2, nb)), dma((max(pairs - 2, 1), nb)),
                dma((pairs, nb)), dma((2, nb)), dma((nb // 2,)), dma((nb // 2,)),
                dma((nb,)), dma((nb,)), dma((nb,)),
                dma((nb,)), dma((nb,)), dma((nb,)),
            ],
            compiler_params=pltpu.CompilerParams(vmem_limit_bytes=67043328, collective_id=0, has_side_effects=True),
            cost_estimate=pl.CostEstimate(flops=flops, bytes_accessed=4 * q.size * 2, transcendentals=0),
        )(q, do, kv)
        shape, kv_shape = queries.shape, keys.shape
        return (odq[:, 0].reshape(shape), odq[:, 1].reshape(shape),
                dkv[:, 0].reshape(kv_shape), dkv[:, 1].reshape(kv_shape))

    return jax.shard_map(local_step, mesh=mesh, in_specs=(part_spec,) * 4, out_specs=(part_spec,) * 4, check_vma=False)
```

```python
import functools
import math

import jax
import jax.numpy as jnp
from jax import lax
from jax.experimental import pallas as pl
from jax.experimental.pallas import tpu as pltpu
from jax.sharding import PartitionSpec as P

NEG_BIG = -1e30
CHUNK = 512
EARLY = 2
AHEAD = 2
FORWARD = 1
NT = (((1,), (1,)), ((), ()))


def mm(a, b):
    return jnp.dot(a, b, preferred_element_type=jnp.float32)


def mm_nt(a, b):
    return lax.dot_general(a, b, NT, preferred_element_type=jnp.float32)


def grad_parts(chip, half, t, bufs, grads):
    pbs, dss, rows_buf = bufs
    c_len = grads.shape[3] // 2

    def part(j, which, buf):
        span = slice(None) if half or j < chip else slice(0, c_len)

        def run():
            grads[j, t, which, span] += mm(buf[half, j, span], rows_buf[half, which])
        return run

    return [part(j, which, buf) for j in range(chip + 1) for which, buf in ((1, pbs), (0, dss))]


def softmax_part(chip, half, r, t, grp, qd, kv, kvt, bufs, fill):
    pbs, dss, rows_buf = bufs
    c_len, d_head = kv.shape[-2:]
    pair = 2 * c_len
    scale = d_head ** -0.5
    k2 = scale * math.log2(math.e)
    n = chip + 1
    fill = list(fill)
    rs = pl.ds(pl.multiple_of(r * CHUNK, CHUNK), CHUNK)
    q = qd[t, half, 0, rs]
    do = qd[t, half, 1, rs]
    rows_buf[half, 0] = q
    rows_buf[half, 1] = do
    span = [pair] * chip + [c_len * (half + 1)]
    tops = [pair * j for j in range(n)]
    n_key = sum(span)
    keys = kv[:n, t, 0].reshape(n * pair, d_head)[:n_key]
    vals = kv[:n, t, 1].reshape(n * pair, d_head)[:n_key]
    s_all = mm_nt(keys, q)
    s = [s_all[a:a + w] for a, w in zip(tops, span)]
    tok = half * c_len + r * (CHUNK // grp) + lax.broadcasted_iota(jnp.int32, (1, CHUNK), 1) // grp
    key_pos = lax.broadcasted_iota(jnp.int32, (span[-1], CHUNK), 0)
    s[-1] = jnp.where(key_pos <= tok, s[-1], NEG_BIG)
    m = functools.reduce(jnp.maximum, [x.max(axis=0, keepdims=True) for x in s])
    mk = m * k2
    p = []
    l = 0.0
    o_t = None
    for j in range(n):
        parts = []
        for a in range(0, span[j], c_len):
            x = jnp.exp2(s[j][a:a + c_len] * k2 - mk)
            l = l + x.sum(axis=0, keepdims=True)
            parts.append(x)
            if fill:
                fill.pop(0)()
        p.append(parts)
        x = [x.astype(jnp.bfloat16) for x in parts]
        part = mm(kvt[j, 1, :, :span[j]], jnp.concatenate(x, axis=0) if len(x) > 1 else x[0])
        o_t = part if o_t is None else o_t + part
    for step in fill:
        step()
    rl = 1.0 / l
    dps = [mm_nt(vals[a:a + w], do) for a, w in list(zip(tops, span))[:EARLY]]
    o_t = (o_t * rl).astype(jnp.bfloat16)
    delta = jnp.sum(do.T.astype(jnp.float32) * o_t.astype(jnp.float32), axis=0, keepdims=True)
    dq_t = None
    for j in range(n):
        if j + EARLY < n:
            a = tops[j + EARLY]
            dps.append(mm_nt(vals[a:a + span[j + EARLY]], do))
        for i, x in enumerate(p[j]):
            at = slice(i * c_len, (i + 1) * c_len)
            x = x * rl
            pbs[half, j, at] = x.astype(jnp.bfloat16)
            dss[half, j, at] = (x * (dps[j][at] - delta)).astype(jnp.bfloat16)
        part = mm(kvt[j, 0, :, :span[j]], dss[half, j, :span[j]])
        dq_t = part if dq_t is None else dq_t + part
    qd[t, half, 0, rs] = o_t.T
    qd[t, half, 1, rs] = (dq_t * scale).astype(jnp.bfloat16).T


def attend(chip, t, grp, qd, kv, kvt, grads, bufs, send_now):
    c_len, d_head = kv.shape[-2:]
    pair = 2 * c_len
    nb = qd.shape[0]
    for j in range(chip + 1):
        kvt[j, 0] = kv[j, t, 0].reshape(pair, d_head).T
        kvt[j, 1] = kv[j, t, 1].reshape(pair, d_head).T
        grads[j, t] = jnp.zeros(grads.shape[2:], jnp.float32)

    def chunk(r, _):
        before = jnp.where(r == 0, jnp.maximum(t - 1, 0), t)
        softmax_part(chip, 0, r, t, grp, qd, kv, kvt, bufs, grad_parts(chip, 1, before, bufs, grads))

        @pl.when((r == 0) & (t >= 1))
        def _():
            send_now(t - 1)

        @pl.when(t < nb)
        def _():
            softmax_part(chip, 1, r, t, grp, qd, kv, kvt, bufs, grad_parts(chip, 0, t, bufs, grads))
        return 0

    lax.fori_loop(0, qd.shape[-2] // CHUNK, chunk, 0)


RELAY = 2
NOW = {0: (), 1: ((0, 0, 0, 1),), 2: ((0, 0, 3, 0), (0, 1, 1, 0), (1, 1, 1, 1)),
       3: ((1, 0, 2, 0), (1, 1, 0, RELAY), (2, 0, 2, 1), (0, 1, 0, 0), (2, 1, 2, 1))}
MERGED = {0: None, 1: (0, 1, 0, 1), 2: (1, 0, 1, 1), 3: (0, 0, 0, 0)}
OWN_SLOTS = {0: (1, 0), 1: (1,), 2: (1,), 3: ()}
LAGS = {0: 6, 1: 4, 2: 2, 3: 2}
RELAY_LAG = 3


def run_chip(chip, n_chip, grp, q_ref, do_ref, k_ref, v_ref, odq_ref, dkv_ref, qd, kv, kvt, grads, inbox, relay,
             pbs, dss, rows_buf, load_sem, pair_send, pair_recv, kv_send, kv_recv, fwd_send, sum_send, sum_recv,
             relay_send, relay_recv,
             out_sem, out_send, out_recv, g_sem, g_send, g_recv):
    nb = qd.shape[0]
    c_len, d_head = kv.shape[-2:]
    scale = d_head ** -0.5
    core = lax.axis_index("ctx") % 2
    last = n_chip - 1
    targets = []
    if chip < last:
        targets.append(chip + 1)
    if chip == 0 and last > 1:
        targets.append(last)

    def dev(to_chip, to_core):
        return {"ctx": 2 * to_chip + to_core}

    def remote(src, dst, send, recv, to):
        return pltpu.make_async_remote_copy(src_ref=src, dst_ref=dst, send_sem=send, recv_sem=recv, device_id=to,
                                            device_id_type=pl.DeviceIdType.MESH)

    def loads(t):
        b = core * nb + t
        return [pltpu.make_async_copy(q_ref.at[b], qd.at[t, core, 0], load_sem.at[0, t]),
                pltpu.make_async_copy(do_ref.at[b], qd.at[t, core, 1], load_sem.at[1, t]),
                pltpu.make_async_copy(k_ref.at[b], kv.at[chip, t, 0, core], load_sem.at[2, t]),
                pltpu.make_async_copy(v_ref.at[b], kv.at[chip, t, 1, core], load_sem.at[3, t])]

    def pair_copies(t, half):
        b = (1 - core) * nb + t
        to = dev(chip, 1 - core)
        return [remote(q_ref.at[b], qd.at[t, half, 0], pair_send.at[0, t], pair_recv.at[0, t], to),
                remote(do_ref.at[b], qd.at[t, half, 1], pair_send.at[1, t], pair_recv.at[1, t], to),
                remote(k_ref.at[b], kv.at[chip, t, 0, half], pair_send.at[2, t], pair_recv.at[2, t], to),
                remote(v_ref.at[b], kv.at[chip, t, 1, half], pair_send.at[3, t], pair_recv.at[3, t], to)]

    def kv_pushes(t):
        out = []
        for i, to_chip in enumerate(targets):
            for other in range(2):
                plane = core if other == 0 else 1 - core
                for w, ref in enumerate((k_ref, v_ref)):
                    out.append(remote(ref.at[plane * nb + t], kv.at[chip, t, w, core], kv_send.at[i, other, w, t],
                                      kv_recv.at[chip, core, w, t], dev(to_chip, plane)))
        return out

    def direct(src):
        return src == chip - 1 or (src == 0 and chip == last)

    def kv_wait(src, t):
        if direct(src):
            for half in range(2):
                for w in range(2):
                    remote(k_ref.at[0], kv.at[src, t, w, half], kv_send.at[0, 0, w, t], kv_recv.at[src, half, w, t],
                           dev(chip, 1 - core)).wait_recv()
        else:
            remote(kv.at[src, t], kv.at[src, t], fwd_send.at[0, t], kv_recv.at[src, 0, 0, t], dev(chip, 1 - core)).wait_recv()

    fwd_srcs = [s for s in range(chip) if chip < last and not (s == 0 and chip + 1 == last)]

    def forward(i, t):
        src = fwd_srcs[i]
        return remote(kv.at[src, t], kv.at[src, t], fwd_send.at[i, t], kv_recv.at[src, 0, 0, t], dev(chip + 1, core))

    def issue(t):
        for c in loads(t) + pair_copies(t, core) + kv_pushes(t):
            c.start()

    def issue_forward(t):
        for i, src in enumerate(fwd_srcs):
            kv_wait(src, t)
            forward(i, t).start()

    def send_sum(route, t):
        d, w, to_chip, slot = route
        if slot == RELAY:
            dst, recv = relay.at[t], relay_recv.at[t]
        else:
            dst, recv = inbox.at[slot, t, w], sum_recv.at[slot, w, t]
        return remote(grads.at[d, t, w], dst, sum_send.at[d, w, t], recv, dev(to_chip, core))

    def relay_on(t):
        return remote(relay.at[t], relay.at[t], relay_send.at[t], relay_recv.at[t], dev(1, core))

    def inbox_wait(slot, w, t):
        ref = inbox.at[slot, t, w]
        remote(ref, ref, sum_send.at[0, w, t], sum_recv.at[slot, w, t], dev(chip, 1 - core)).wait_recv()

    def outs(t):
        b = core * nb + t
        return [pltpu.make_async_copy(qd.at[t, core], odq_ref.at[b], out_sem.at[t]),
                remote(qd.at[t, 1 - core], odq_ref.at[b], out_send.at[t], out_recv.at[t], dev(chip, 1 - core))]

    def grad_outs(t):
        b = core * nb + t
        return [pltpu.make_async_copy(kv.at[chip, t, :, core], dkv_ref.at[b], g_sem.at[t]),
                remote(kv.at[chip, t, :, 1 - core], dkv_ref.at[b], g_send.at[t], g_recv.at[t], dev(chip, 1 - core))]

    def send_now(t):
        for route in NOW[chip]:
            send_sum(route, t).start()

    def pass_relay(t):
        relay_on(t).wait_recv()
        relay_on(t).start()

    def reduce_step(t):
        if MERGED[chip]:
            d, w = MERGED[chip][:2]
            inbox_wait(0, w, t)
            grads[d, t, w] += inbox[0, t, w]
            send_sum(MERGED[chip], t).start()
        total = [grads[chip, t, 0], grads[chip, t, 1]]
        for slot in OWN_SLOTS[chip]:
            for w in range(2):
                inbox_wait(slot, w, t)
                total[w] = total[w] + inbox[slot, t, w]
        if chip == 1:
            relay_on(t).wait_recv()
            total[1] = total[1] + relay[t]
        block = (2, c_len, d_head)
        kv[chip, t, 0] = (total[0] * scale).astype(jnp.bfloat16).reshape(block)
        kv[chip, t, 1] = total[1].astype(jnp.bfloat16).reshape(block)
        for c in grad_outs(t):
            c.start()

    lag = LAGS[chip]
    bufs = (pbs, dss, rows_buf)
    for ref in bufs:
        ref[...] = jnp.zeros(ref.shape, ref.dtype)

    def prologue(t, _):
        issue(t)
        return 0

    lax.fori_loop(0, AHEAD, prologue, 0)
    if fwd_srcs:
        def fwd_prologue(t, _):
            issue_forward(t)
            return 0
        lax.fori_loop(0, FORWARD, fwd_prologue, 0)

    def step(t, _):
        @pl.when(t + AHEAD < nb)
        def _():
            issue(t + AHEAD)
        if fwd_srcs:
            @pl.when(t + FORWARD < nb)
            def _():
                issue_forward(t + FORWARD)
        for c in loads(t):
            c.wait()
        for c in pair_copies(t, 1 - core):
            c.wait_recv()
        for src in range(chip):
            if src not in fwd_srcs:
                kv_wait(src, t)
        attend(chip, t, grp, qd, kv, kvt, grads, bufs, send_now)
        for c in outs(t):
            c.start()

        if chip == 0:
            @pl.when(t >= RELAY_LAG)
            def _():
                pass_relay(t - RELAY_LAG)

        @pl.when(t >= lag)
        def _():
            reduce_step(t - lag)
        return 0

    lax.fori_loop(0, nb, step, 0)
    for part in grad_parts(chip, 1, nb - 1, bufs, grads):
        part()
    send_now(nb - 1)

    def relay_tail(t, _):
        pass_relay(t)
        return 0

    if chip == 0:
        lax.fori_loop(nb - RELAY_LAG, nb, relay_tail, 0)

    def tail(t, _):
        reduce_step(t)
        return 0

    lax.fori_loop(nb - lag, nb, tail, 0)

    def drain(t, _):
        for c in pair_copies(t, core) + kv_pushes(t):
            c.wait_send()
        for i in range(len(fwd_srcs)):
            forward(i, t).wait_send()
        for route in NOW[chip] + ((MERGED[chip],) if MERGED[chip] else ()):
            send_sum(route, t).wait_send()
        if chip == 0:
            relay_on(t).wait_send()
        b = (1 - core) * nb + t
        for local, away in (outs(t), grad_outs(t)):
            local.wait()
            away.wait_send()
        remote(qd.at[t, core], odq_ref.at[b], out_send.at[t], out_recv.at[t], dev(chip, 1 - core)).wait_recv()
        remote(kv.at[chip, t, :, core], dkv_ref.at[b], g_send.at[t], g_recv.at[t], dev(chip, 1 - core)).wait_recv()
        return 0

    lax.fori_loop(0, nb, drain, 0)


def kernel(n_chip, grp, *refs):
    me = lax.axis_index("ctx")
    barrier = pltpu.get_barrier_semaphore()
    for i in range(1, 2 * n_chip):
        pl.semaphore_signal(barrier, inc=1, device_id={"ctx": lax.rem(me + i, 2 * n_chip)},
                            device_id_type=pl.DeviceIdType.MESH)
    pl.semaphore_wait(barrier, 2 * n_chip - 1)
    for chip in range(n_chip):
        @pl.when(me // 2 == chip)
        def _():
            run_chip(chip, n_chip, grp, *refs)


def solution(mesh):
    part_spec = P("dp", "ctx")
    n_chip = mesh.shape["ctx"] // 2

    def local_step(queries, keys, values, grad_out):
        n_batch, c_len, n_q, d_head = queries.shape
        rows = c_len * n_q
        nb = n_batch // 2
        q = queries.reshape(n_batch, rows, d_head)
        do = grad_out.reshape(n_batch, rows, d_head)
        k = keys.reshape(n_batch, c_len, d_head)
        v = values.reshape(n_batch, c_len, d_head)
        dma = pltpu.SemaphoreType.DMA
        any_spec = pl.BlockSpec(memory_space=pl.ANY)
        pairs = n_chip
        flops = 2 * nb * 2 * rows * n_chip * 2 * c_len * d_head * 6
        odq, dkv = pl.pallas_call(
            functools.partial(kernel, n_chip, n_q),
            in_specs=[any_spec] * 4,
            out_specs=[any_spec] * 2,
            out_shape=[jax.ShapeDtypeStruct((n_batch, 2, rows, d_head), jnp.bfloat16),
                       jax.ShapeDtypeStruct((n_batch, 2, c_len, d_head), jnp.bfloat16)],
            scratch_shapes=[
                pltpu.VMEM((nb, 2, 2, rows, d_head), jnp.bfloat16),
                pltpu.VMEM((pairs, nb, 2, 2, c_len, d_head), jnp.bfloat16),
                pltpu.VMEM((pairs, 2, d_head, 2 * c_len), jnp.bfloat16),
                pltpu.VMEM((pairs, nb, 2, 2 * c_len, d_head), jnp.float32),
                pltpu.VMEM((2, nb, 2, 2 * c_len, d_head), jnp.float32),
                pltpu.VMEM((nb, 2 * c_len, d_head), jnp.float32),
                pltpu.VMEM((2, pairs, 2 * c_len, CHUNK), jnp.bfloat16),
                pltpu.VMEM((2, pairs, 2 * c_len, CHUNK), jnp.bfloat16),
                pltpu.VMEM((2, 2, CHUNK, d_head), jnp.bfloat16),
                dma((4, nb)), dma((4, nb)), dma((4, nb)),
                dma((2, 2, 2, nb)), dma((pairs, 2, 2, nb)), dma((max(pairs - 2, 1), nb)),
                dma((pairs, 2, nb)), dma((2, 2, nb)), dma((nb,)), dma((nb,)),
                dma((nb,)), dma((nb,)), dma((nb,)),
                dma((nb,)), dma((nb,)), dma((nb,)),
            ],
            compiler_params=pltpu.CompilerParams(vmem_limit_bytes=67043328, collective_id=0, has_side_effects=True),
            cost_estimate=pl.CostEstimate(flops=flops, bytes_accessed=4 * q.size * 2, transcendentals=0),
        )(q, do, k, v)
        shape, kv_shape = queries.shape, keys.shape
        return (odq[:, 0].reshape(shape), odq[:, 1].reshape(shape),
                dkv[:, 0].reshape(kv_shape), dkv[:, 1].reshape(kv_shape))

    return jax.shard_map(local_step, mesh=mesh, in_specs=(part_spec,) * 4, out_specs=(part_spec,) * 4, check_vma=False)
```

```python
import functools
import math

import jax
import jax.numpy as jnp
from jax import lax
from jax.experimental import pallas as pl
from jax.experimental.pallas import tpu as pltpu
from jax.sharding import PartitionSpec as P

NEG_BIG = -1e30
CHUNK = 512
EARLY = 2
AHEAD = 2
FORWARD = 1
NT = (((1,), (1,)), ((), ()))


def mm(a, b):
    return jnp.dot(a, b, preferred_element_type=jnp.float32)


def mm_nt(a, b):
    return lax.dot_general(a, b, NT, preferred_element_type=jnp.float32)


def grad_parts(chip, half, t, bufs, grads):
    pbs, dss, rows_buf = bufs
    c_len = grads.shape[3] // 2

    def part(j, which, buf):
        span = slice(None) if half or j < chip else slice(0, c_len)

        def run():
            grads[j, t, which, span] += mm(buf[half, j, span], rows_buf[half, which])
        return run

    return [part(j, which, buf) for j in range(chip + 1) for which, buf in ((1, pbs), (0, dss))]


def softmax_part(chip, half, r, t, grp, qd, kv, kvt, bufs, fill):
    pbs, dss, rows_buf = bufs
    c_len, d_head = kv.shape[-2:]
    pair = 2 * c_len
    scale = d_head ** -0.5
    k2 = scale * math.log2(math.e)
    n = chip + 1
    fill = list(fill)
    rs = pl.ds(r * CHUNK, CHUNK)
    q = qd[t, half, 0, rs]
    do = qd[t, half, 1, rs]
    rows_buf[half, 0] = q
    rows_buf[half, 1] = do
    span = [pair] * chip + [c_len * (half + 1)]
    tops = [pair * j for j in range(n)]
    n_key = sum(span)
    keys = kv[:n, t, 0].reshape(n * pair, d_head)[:n_key]
    vals = kv[:n, t, 1].reshape(n * pair, d_head)[:n_key]
    s_all = mm_nt(keys, q)
    s = [s_all[a:a + w] for a, w in zip(tops, span)]
    tok = half * c_len + r * (CHUNK // grp) + lax.broadcasted_iota(jnp.int32, (1, CHUNK), 1) // grp
    key_pos = lax.broadcasted_iota(jnp.int32, (span[-1], CHUNK), 0)
    s[-1] = jnp.where(key_pos <= tok, s[-1], NEG_BIG)
    m = functools.reduce(jnp.maximum, [x.max(axis=0, keepdims=True) for x in s])
    mk = m * k2
    p = []
    l = 0.0
    o_t = None
    for j in range(n):
        parts = []
        for a in range(0, span[j], c_len):
            x = jnp.exp2(s[j][a:a + c_len] * k2 - mk)
            l = l + x.sum(axis=0, keepdims=True)
            parts.append(x)
            if fill:
                fill.pop(0)()
        p.append(parts)
        x = [x.astype(jnp.bfloat16) for x in parts]
        part = mm(kvt[j, 1, :, :span[j]], jnp.concatenate(x, axis=0) if len(x) > 1 else x[0])
        o_t = part if o_t is None else o_t + part
    for step in fill:
        step()
    rl = 1.0 / l
    dps = [mm_nt(vals[a:a + w], do) for a, w in list(zip(tops, span))[:EARLY]]
    o_t = (o_t * rl).astype(jnp.bfloat16)
    delta = jnp.sum(do.T.astype(jnp.float32) * o_t.astype(jnp.float32), axis=0, keepdims=True)
    dq_t = None
    for j in range(n):
        if j + EARLY < n:
            a = tops[j + EARLY]
            dps.append(mm_nt(vals[a:a + span[j + EARLY]], do))
        for i, x in enumerate(p[j]):
            at = slice(i * c_len, (i + 1) * c_len)
            x = x * rl
            pbs[half, j, at] = x.astype(jnp.bfloat16)
            dss[half, j, at] = (x * (dps[j][at] - delta)).astype(jnp.bfloat16)
        part = mm(kvt[j, 0, :, :span[j]], dss[half, j, :span[j]])
        dq_t = part if dq_t is None else dq_t + part
    qd[t, half, 0, rs] = o_t.T
    qd[t, half, 1, rs] = (dq_t * scale).astype(jnp.bfloat16).T


def attend(chip, t, grp, qd, kv, kvt, grads, bufs, send_now):
    c_len, d_head = kv.shape[-2:]
    pair = 2 * c_len
    nb = qd.shape[0]
    for j in range(chip + 1):
        kvt[j, 0] = kv[j, t, 0].reshape(pair, d_head).T
        kvt[j, 1] = kv[j, t, 1].reshape(pair, d_head).T
        grads[j, t] = jnp.zeros(grads.shape[2:], jnp.float32)

    def second(r):
        @pl.when(t < nb)
        def _():
            softmax_part(chip, 1, r, t, grp, qd, kv, kvt, bufs, grad_parts(chip, 0, t, bufs, grads))

    def first(r):
        before = jnp.maximum(t - 1, 0) if r == 0 else t
        softmax_part(chip, 0, r, t, grp, qd, kv, kvt, bufs, grad_parts(chip, 1, before, bufs, grads))

    first(0)

    @pl.when(t >= 1)
    def _():
        send_now(t - 1)

    second(0)
    for r in range(1, qd.shape[-2] // CHUNK):
        pl.when(t < nb)(functools.partial(first, r))
        second(r)


RELAY = 2
NOW = {0: (), 1: ((0, 0, 0, 1),), 2: ((0, 0, 3, 0), (0, 1, 1, 0), (1, 1, 1, 1)),
       3: ((1, 0, 2, 0), (1, 1, 0, RELAY), (2, 0, 2, 1), (0, 1, 0, 0), (2, 1, 2, 1))}
MERGED = {0: None, 1: (0, 1, 0, 1), 2: (1, 0, 1, 1), 3: (0, 0, 0, 0)}
OWN_SLOTS = {0: (1, 0), 1: (1,), 2: (1,), 3: ()}
LAGS = {0: 6, 1: 4, 2: 2, 3: 2}
RELAY_LAG = 3


def run_chip(chip, n_chip, grp, q_ref, do_ref, k_ref, v_ref, odq_ref, dkv_ref, qd, kv, kvt, grads, inbox, relay,
             pbs, dss, rows_buf, load_sem, pair_send, pair_recv, kv_send, kv_recv, fwd_send, sum_send, sum_recv,
             relay_send, relay_recv,
             out_sem, out_send, out_recv, g_sem, g_send, g_recv):
    nb = qd.shape[0]
    c_len, d_head = kv.shape[-2:]
    scale = d_head ** -0.5
    core = lax.axis_index("ctx") % 2
    last = n_chip - 1
    targets = []
    if chip < last:
        targets.append(chip + 1)
    if chip == 0 and last > 1:
        targets.append(last)

    def dev(to_chip, to_core):
        return {"ctx": 2 * to_chip + to_core}

    def remote(src, dst, send, recv, to):
        return pltpu.make_async_remote_copy(src_ref=src, dst_ref=dst, send_sem=send, recv_sem=recv, device_id=to,
                                            device_id_type=pl.DeviceIdType.MESH)

    def loads(t):
        b = core * nb + t
        return [pltpu.make_async_copy(q_ref.at[b], qd.at[t, core, 0], load_sem.at[0, t]),
                pltpu.make_async_copy(do_ref.at[b], qd.at[t, core, 1], load_sem.at[1, t]),
                pltpu.make_async_copy(k_ref.at[b], kv.at[chip, t, 0, core], load_sem.at[2, t]),
                pltpu.make_async_copy(v_ref.at[b], kv.at[chip, t, 1, core], load_sem.at[3, t])]

    def pair_copies(t, half):
        b = (1 - core) * nb + t
        to = dev(chip, 1 - core)
        return [remote(q_ref.at[b], qd.at[t, half, 0], pair_send.at[0, t], pair_recv.at[0, t], to),
                remote(do_ref.at[b], qd.at[t, half, 1], pair_send.at[1, t], pair_recv.at[1, t], to),
                remote(k_ref.at[b], kv.at[chip, t, 0, half], pair_send.at[2, t], pair_recv.at[2, t], to),
                remote(v_ref.at[b], kv.at[chip, t, 1, half], pair_send.at[3, t], pair_recv.at[3, t], to)]

    def kv_pushes(t):
        out = []
        for i, to_chip in enumerate(targets):
            for other in range(2):
                plane = core if other == 0 else 1 - core
                for w, ref in enumerate((k_ref, v_ref)):
                    out.append(remote(ref.at[plane * nb + t], kv.at[chip, t, w, core], kv_send.at[i, other, w, t],
                                      kv_recv.at[chip, core, w, t], dev(to_chip, plane)))
        return out

    def direct(src):
        return src == chip - 1 or (src == 0 and chip == last)

    def kv_wait(src, t):
        if direct(src):
            for half in range(2):
                for w in range(2):
                    remote(k_ref.at[0], kv.at[src, t, w, half], kv_send.at[0, 0, w, t], kv_recv.at[src, half, w, t],
                           dev(chip, 1 - core)).wait_recv()
        else:
            remote(kv.at[src, t], kv.at[src, t], fwd_send.at[0, t], kv_recv.at[src, 0, 0, t], dev(chip, 1 - core)).wait_recv()

    fwd_srcs = [s for s in range(chip) if chip < last and not (s == 0 and chip + 1 == last)]

    def forward(i, t):
        src = fwd_srcs[i]
        return remote(kv.at[src, t], kv.at[src, t], fwd_send.at[i, t], kv_recv.at[src, 0, 0, t], dev(chip + 1, core))

    def issue(t):
        for c in loads(t) + pair_copies(t, core) + kv_pushes(t):
            c.start()

    def issue_forward(t):
        for i, src in enumerate(fwd_srcs):
            kv_wait(src, t)
            forward(i, t).start()

    def send_sum(route, t):
        d, w, to_chip, slot = route
        if slot == RELAY:
            dst, recv = relay.at[t], relay_recv.at[t]
        else:
            dst, recv = inbox.at[slot, t, w], sum_recv.at[slot, w, t]
        return remote(grads.at[d, t, w], dst, sum_send.at[d, w, t], recv, dev(to_chip, core))

    def relay_on(t):
        return remote(relay.at[t], relay.at[t], relay_send.at[t], relay_recv.at[t], dev(1, core))

    def inbox_wait(slot, w, t):
        ref = inbox.at[slot, t, w]
        remote(ref, ref, sum_send.at[0, w, t], sum_recv.at[slot, w, t], dev(chip, 1 - core)).wait_recv()

    def outs(t):
        b = core * nb + t
        return [pltpu.make_async_copy(qd.at[t, core], odq_ref.at[b], out_sem.at[t]),
                remote(qd.at[t, 1 - core], odq_ref.at[b], out_send.at[t], out_recv.at[t], dev(chip, 1 - core))]

    def grad_outs(t):
        b = core * nb + t
        return [pltpu.make_async_copy(kv.at[chip, t, :, core], dkv_ref.at[b], g_sem.at[t]),
                remote(kv.at[chip, t, :, 1 - core], dkv_ref.at[b], g_send.at[t], g_recv.at[t], dev(chip, 1 - core))]

    def send_now(t):
        for route in NOW[chip]:
            send_sum(route, t).start()

    def pass_relay(t):
        relay_on(t).wait_recv()
        relay_on(t).start()

    def reduce_step(t):
        if MERGED[chip]:
            d, w = MERGED[chip][:2]
            inbox_wait(0, w, t)
            grads[d, t, w] += inbox[0, t, w]
            send_sum(MERGED[chip], t).start()
        total = [grads[chip, t, 0], grads[chip, t, 1]]
        for slot in OWN_SLOTS[chip]:
            for w in range(2):
                inbox_wait(slot, w, t)
                total[w] = total[w] + inbox[slot, t, w]
        if chip == 1:
            relay_on(t).wait_recv()
            total[1] = total[1] + relay[t]
        block = (2, c_len, d_head)
        kv[chip, t, 0] = (total[0] * scale).astype(jnp.bfloat16).reshape(block)
        kv[chip, t, 1] = total[1].astype(jnp.bfloat16).reshape(block)
        for c in grad_outs(t):
            c.start()

    lag = LAGS[chip]
    bufs = (pbs, dss, rows_buf)

    def prologue(t, _):
        issue(t)
        return 0

    lax.fori_loop(0, AHEAD, prologue, 0)
    if fwd_srcs:
        def fwd_prologue(t, _):
            issue_forward(t)
            return 0
        lax.fori_loop(0, FORWARD, fwd_prologue, 0)

    for ref in bufs:
        ref[...] = jnp.zeros(ref.shape, ref.dtype)

    def step(t, _):
        @pl.when(t + AHEAD < nb)
        def _():
            issue(t + AHEAD)
        if fwd_srcs:
            @pl.when(t + FORWARD < nb)
            def _():
                issue_forward(t + FORWARD)
        for c in loads(t):
            c.wait()
        for c in pair_copies(t, 1 - core):
            c.wait_recv()
        for src in range(chip):
            if src not in fwd_srcs:
                kv_wait(src, t)
        attend(chip, t, grp, qd, kv, kvt, grads, bufs, send_now)
        for c in outs(t):
            c.start()

        if chip == 0:
            @pl.when(t >= RELAY_LAG)
            def _():
                pass_relay(t - RELAY_LAG)

        @pl.when(t >= lag)
        def _():
            reduce_step(t - lag)
        return 0

    lax.fori_loop(0, nb, step, 0)
    for part in grad_parts(chip, 1, nb - 1, bufs, grads):
        part()
    send_now(nb - 1)

    def relay_tail(t, _):
        pass_relay(t)
        return 0

    if chip == 0:
        lax.fori_loop(nb - RELAY_LAG, nb, relay_tail, 0)

    def tail(t, _):
        reduce_step(t)
        return 0

    lax.fori_loop(nb - lag, nb, tail, 0)

    def drain(t, _):
        for c in pair_copies(t, core) + kv_pushes(t):
            c.wait_send()
        for i in range(len(fwd_srcs)):
            forward(i, t).wait_send()
        for route in NOW[chip] + ((MERGED[chip],) if MERGED[chip] else ()):
            send_sum(route, t).wait_send()
        if chip == 0:
            relay_on(t).wait_send()
        b = (1 - core) * nb + t
        for local, away in (outs(t), grad_outs(t)):
            local.wait()
            away.wait_send()
        remote(qd.at[t, core], odq_ref.at[b], out_send.at[t], out_recv.at[t], dev(chip, 1 - core)).wait_recv()
        remote(kv.at[chip, t, :, core], dkv_ref.at[b], g_send.at[t], g_recv.at[t], dev(chip, 1 - core)).wait_recv()
        return 0

    lax.fori_loop(0, nb, drain, 0)


def kernel(n_chip, grp, *refs):
    me = lax.axis_index("ctx")
    barrier = pltpu.get_barrier_semaphore()
    for i in range(1, 2 * n_chip):
        pl.semaphore_signal(barrier, inc=1, device_id={"ctx": lax.rem(me + i, 2 * n_chip)},
                            device_id_type=pl.DeviceIdType.MESH)
    pl.semaphore_wait(barrier, 2 * n_chip - 1)
    for chip in range(n_chip):
        @pl.when(me // 2 == chip)
        def _():
            run_chip(chip, n_chip, grp, *refs)


def solution(mesh):
    part_spec = P("dp", "ctx")
    n_chip = mesh.shape["ctx"] // 2

    def local_step(queries, keys, values, grad_out):
        n_batch, c_len, n_q, d_head = queries.shape
        rows = c_len * n_q
        nb = n_batch // 2
        q = queries.reshape(n_batch, rows, d_head)
        do = grad_out.reshape(n_batch, rows, d_head)
        k = keys.reshape(n_batch, c_len, d_head)
        v = values.reshape(n_batch, c_len, d_head)
        dma = pltpu.SemaphoreType.DMA
        any_spec = pl.BlockSpec(memory_space=pl.ANY)
        pairs = n_chip
        flops = 2 * nb * 2 * rows * n_chip * 2 * c_len * d_head * 6
        odq, dkv = pl.pallas_call(
            functools.partial(kernel, n_chip, n_q),
            in_specs=[any_spec] * 4,
            out_specs=[any_spec] * 2,
            out_shape=[jax.ShapeDtypeStruct((n_batch, 2, rows, d_head), jnp.bfloat16),
                       jax.ShapeDtypeStruct((n_batch, 2, c_len, d_head), jnp.bfloat16)],
            scratch_shapes=[
                pltpu.VMEM((nb, 2, 2, rows, d_head), jnp.bfloat16),
                pltpu.VMEM((pairs, nb, 2, 2, c_len, d_head), jnp.bfloat16),
                pltpu.VMEM((pairs, 2, d_head, 2 * c_len), jnp.bfloat16),
                pltpu.VMEM((pairs, nb, 2, 2 * c_len, d_head), jnp.float32),
                pltpu.VMEM((2, nb, 2, 2 * c_len, d_head), jnp.float32),
                pltpu.VMEM((nb, 2 * c_len, d_head), jnp.float32),
                pltpu.VMEM((2, pairs, 2 * c_len, CHUNK), jnp.bfloat16),
                pltpu.VMEM((2, pairs, 2 * c_len, CHUNK), jnp.bfloat16),
                pltpu.VMEM((2, 2, CHUNK, d_head), jnp.bfloat16),
                dma((4, nb)), dma((4, nb)), dma((4, nb)),
                dma((2, 2, 2, nb)), dma((pairs, 2, 2, nb)), dma((max(pairs - 2, 1), nb)),
                dma((pairs, 2, nb)), dma((2, 2, nb)), dma((nb,)), dma((nb,)),
                dma((nb,)), dma((nb,)), dma((nb,)),
                dma((nb,)), dma((nb,)), dma((nb,)),
            ],
            compiler_params=pltpu.CompilerParams(vmem_limit_bytes=67043328, collective_id=0, has_side_effects=True),
            cost_estimate=pl.CostEstimate(flops=flops, bytes_accessed=4 * q.size * 2, transcendentals=0),
        )(q, do, k, v)
        shape, kv_shape = queries.shape, keys.shape
        return (odq[:, 0].reshape(shape), odq[:, 1].reshape(shape),
                dkv[:, 0].reshape(kv_shape), dkv[:, 1].reshape(kv_shape))

    return jax.shard_map(local_step, mesh=mesh, in_specs=(part_spec,) * 4, out_specs=(part_spec,) * 4, check_vma=False)
```
